32 devices in a mesh: dp: 2 (over x), cfg: 4 (over z), tp: 4 (over y, core).
Axes of the slice: x: 2, y: 2, z: 4, core: 2. Of those that a mesh axis runs over, the one named last changes fastest.
Arguments:
- hidden: bfloat16 [32, 1024, 1152], P(('dp', 'cfg')), parts along dimension 0
- caption: bfloat16 [32, 300, 1152], P(('dp', 'cfg')), parts along dimension 0
- cap_len: int32 [32], P(('dp', 'cfg')), parts along dimension 0
- t_block: bfloat16 [16, 6912], P('dp'), parts along dimension 0
- t_embed: bfloat16 [16, 1152], P('dp'), parts along dimension 0
- x_t: float32 [16, 64, 64, 4], P('dp'), parts along dimension 0
- alpha_bar: float32 [16, 2], P('dp'), parts along dimension 0
- mod_table: bfloat16 [2, 6, 1152], replicated
- w_qkv: bfloat16 [2, 1152, 3, 16, 72], P(None, None, None, 'tp')
- w_proj: bfloat16 [2, 16, 72, 1152], P(None, 'tp')
- w_cq: bfloat16 [2, 1152, 16, 72], P(None, None, 'tp')
- w_ckv: bfloat16 [2, 1152, 2, 16, 72], P(None, None, None, 'tp')
- w_cproj: bfloat16 [2, 16, 72, 1152], P(None, 'tp')
- w_fc1: bfloat16 [2, 1152, 4608], P(None, None, 'tp')
- w_fc2: bfloat16 [2, 4608, 1152], P(None, 'tp')
- final_table: bfloat16 [2, 1152], replicated
- w_out: bfloat16 [1152, 32], replicated
- b_out: bfloat16 [32], replicated
Outputs:
- output: float32 [16, 64, 64, 4], P('dp'), parts along dimension 0
There are 2 independent parts. The reference program is written for one: setup_inputs(seed, part) draws one part's arguments, and reference() takes and returns one part's arrays. A program takes and returns all parts, laid end to end along the dimension named above; an argument that names none is the same for every part.
All inputs are finite; a program needn't handle non-finite values.
Results may differ from the reference program's by a relative error of at most 0.0137388.
Values are sent between devices in bfloat16 or wider.
A program may use at most 1 GiB of HBM per device.

```python
import jax
import jax.numpy as jnp
from jax import lax

BATCH_SIZE = 8
LATENT_SIDE = 64
MODEL_DIM = 1152
NUM_HEADS = 16
TEXT_LEN = 300
HIDDEN_FF = 4608

NUM_TOKENS = (LATENT_SIDE // 2) * (LATENT_SIDE // 2)
HEAD_DIM = MODEL_DIM // NUM_HEADS
GUIDANCE = 4.5
LN_EPS = 1e-6


def setup_inputs(seed: int = 0, part: int = 0) -> dict:
    part_keys = jax.random.split(jax.random.fold_in(jax.random.key(seed), part), 10)
    weight_keys = jax.random.split(jax.random.key(seed + 1), 11)
    total_rows = 2 * BATCH_SIZE
    common = jax.random.normal(part_keys[0], (total_rows, 1, MODEL_DIM), jnp.float32)
    tok_noise = jax.random.normal(part_keys[1], (total_rows, NUM_TOKENS, MODEL_DIM), jnp.float32)
    hidden = common + tok_noise
    cap_mean = jax.random.normal(part_keys[2], (total_rows, 1, MODEL_DIM), jnp.float32)
    caption = cap_mean + jax.random.normal(part_keys[3], (total_rows, TEXT_LEN, MODEL_DIM), jnp.float32)
    len_keys = jax.random.split(part_keys[4], 2)
    cond_len = jax.random.randint(len_keys[0], (BATCH_SIZE,), TEXT_LEN // 4, TEXT_LEN + 1)
    uncond_len = jax.random.randint(len_keys[1], (BATCH_SIZE,), 1, TEXT_LEN // 16 + 2)
    cap_len = jnp.concatenate([cond_len.at[0].set(TEXT_LEN), uncond_len]).astype(jnp.int32)
    t_block = 0.5 * jax.random.normal(part_keys[5], (BATCH_SIZE, 6 * MODEL_DIM), jnp.float32)
    t_embed = 0.5 * jax.random.normal(part_keys[6], (BATCH_SIZE, MODEL_DIM), jnp.float32)
    x_t = jax.random.normal(part_keys[7], (BATCH_SIZE, LATENT_SIDE, LATENT_SIDE, 4), jnp.float32)
    abar_t = jax.random.uniform(part_keys[8], (BATCH_SIZE,), jnp.float32, 0.15, 0.6)
    abar_gap = jax.random.uniform(part_keys[9], (BATCH_SIZE,), jnp.float32, 0.1, 0.3)
    alpha_bar = jnp.stack([abar_t, abar_t + abar_gap], axis=1)
    dim_scale = MODEL_DIM ** -0.5
    ff_scale = HIDDEN_FF ** -0.5
    mod_table = 0.5 * jax.random.normal(weight_keys[0], (2, 6, MODEL_DIM), jnp.float32)
    w_qkv = dim_scale * jax.random.normal(weight_keys[1], (2, MODEL_DIM, 3, NUM_HEADS, HEAD_DIM), jnp.float32)
    w_proj = dim_scale * jax.random.normal(weight_keys[2], (2, NUM_HEADS, HEAD_DIM, MODEL_DIM), jnp.float32)
    w_cq = dim_scale * jax.random.normal(weight_keys[3], (2, MODEL_DIM, NUM_HEADS, HEAD_DIM), jnp.float32)
    w_ckv = dim_scale * jax.random.normal(weight_keys[4], (2, MODEL_DIM, 2, NUM_HEADS, HEAD_DIM), jnp.float32)
    w_cproj = dim_scale * jax.random.normal(weight_keys[5], (2, NUM_HEADS, HEAD_DIM, MODEL_DIM), jnp.float32)
    w_fc1 = dim_scale * jax.random.normal(weight_keys[6], (2, MODEL_DIM, HIDDEN_FF), jnp.float32)
    w_fc2 = ff_scale * jax.random.normal(weight_keys[7], (2, HIDDEN_FF, MODEL_DIM), jnp.float32)
    final_table = 0.5 * jax.random.normal(weight_keys[8], (2, MODEL_DIM), jnp.float32)
    w_out = dim_scale * jax.random.normal(weight_keys[9], (MODEL_DIM, 32), jnp.float32)
    b_out = 0.3 * jax.random.normal(weight_keys[10], (32,), jnp.float32)
    return {
        'hidden': hidden.astype(jnp.bfloat16),
        'caption': caption.astype(jnp.bfloat16),
        'cap_len': cap_len,
        't_block': t_block.astype(jnp.bfloat16),
        't_embed': t_embed.astype(jnp.bfloat16),
        'x_t': x_t,
        'alpha_bar': alpha_bar,
        'mod_table': mod_table.astype(jnp.bfloat16),
        'w_qkv': w_qkv.astype(jnp.bfloat16),
        'w_proj': w_proj.astype(jnp.bfloat16),
        'w_cq': w_cq.astype(jnp.bfloat16),
        'w_ckv': w_ckv.astype(jnp.bfloat16),
        'w_cproj': w_cproj.astype(jnp.bfloat16),
        'w_fc1': w_fc1.astype(jnp.bfloat16),
        'w_fc2': w_fc2.astype(jnp.bfloat16),
        'final_table': final_table.astype(jnp.bfloat16),
        'w_out': w_out.astype(jnp.bfloat16),
        'b_out': b_out.astype(jnp.bfloat16),
    }


def layer_norm(values):
    mean_val = jnp.mean(values, axis=-1, keepdims=True)
    centered = values - mean_val
    variance = jnp.mean(centered * centered, axis=-1, keepdims=True)
    return centered * lax.rsqrt(variance + LN_EPS)


def attend(queries, key_vecs, values, key_mask):
    def one_head(head_in):
        q_head, k_head, v_head = head_in
        scores = jnp.dot(q_head, k_head.T, preferred_element_type=jnp.float32) * HEAD_DIM ** -0.5
        scores = jnp.where(key_mask[None, :], scores, -1e30)
        attn_prob = jax.nn.softmax(scores, axis=-1).astype(jnp.bfloat16)
        return jnp.dot(attn_prob, v_head, preferred_element_type=jnp.float32).astype(jnp.bfloat16)
    per_head = lax.map(one_head, (jnp.swapaxes(queries, 0, 1), jnp.swapaxes(key_vecs, 0, 1), jnp.swapaxes(values, 0, 1)))
    return jnp.swapaxes(per_head, 0, 1)


def block_row(residual, caption_row, key_mask, t_mods, layer_w):
    mod_tab, w_qkv, w_proj, w_cq, w_ckv, w_cproj, w_fc1, w_fc2 = layer_w
    mod_rows = mod_tab.astype(jnp.float32) + t_mods
    all_keys = jnp.ones((NUM_TOKENS,), jnp.bool_)
    attn_in = (layer_norm(residual) * (1.0 + mod_rows[1]) + mod_rows[0]).astype(jnp.bfloat16)
    qkv_out = jnp.dot(attn_in, w_qkv.reshape(MODEL_DIM, 3 * MODEL_DIM), preferred_element_type=jnp.float32)
    qkv_out = qkv_out.astype(jnp.bfloat16).reshape(NUM_TOKENS, 3, NUM_HEADS, HEAD_DIM)
    self_o = attend(qkv_out[:, 0], qkv_out[:, 1], qkv_out[:, 2], all_keys)
    self_proj = jnp.dot(self_o.reshape(NUM_TOKENS, MODEL_DIM), w_proj.reshape(MODEL_DIM, MODEL_DIM), preferred_element_type=jnp.float32).astype(jnp.bfloat16)
    residual = residual + mod_rows[2] * self_proj.astype(jnp.float32)
    cross_q = jnp.dot(residual.astype(jnp.bfloat16), w_cq.reshape(MODEL_DIM, MODEL_DIM), preferred_element_type=jnp.float32)
    cross_q = cross_q.astype(jnp.bfloat16).reshape(NUM_TOKENS, NUM_HEADS, HEAD_DIM)
    cross_kv = jnp.dot(caption_row, w_ckv.reshape(MODEL_DIM, 2 * MODEL_DIM), preferred_element_type=jnp.float32)
    cross_kv = cross_kv.astype(jnp.bfloat16).reshape(TEXT_LEN, 2, NUM_HEADS, HEAD_DIM)
    cross_o = attend(cross_q, cross_kv[:, 0], cross_kv[:, 1], key_mask)
    cross_proj = jnp.dot(cross_o.reshape(NUM_TOKENS, MODEL_DIM), w_cproj.reshape(MODEL_DIM, MODEL_DIM), preferred_element_type=jnp.float32).astype(jnp.bfloat16)
    residual = residual + cross_proj.astype(jnp.float32)
    mlp_in = (layer_norm(residual) * (1.0 + mod_rows[4]) + mod_rows[3]).astype(jnp.bfloat16)
    mlp_hidden = jax.nn.gelu(jnp.dot(mlp_in, w_fc1, preferred_element_type=jnp.float32), approximate=True).astype(jnp.bfloat16)
    mlp_out = jnp.dot(mlp_hidden, w_fc2, preferred_element_type=jnp.float32).astype(jnp.bfloat16)
    return residual + mod_rows[5] * mlp_out.astype(jnp.float32)


def reference(hidden, caption, cap_len, t_block, t_embed, x_t, alpha_bar, mod_table, w_qkv, w_proj, w_cq, w_ckv, w_cproj, w_fc1, w_fc2, final_table, w_out, b_out):
    t_rows = jnp.tile(t_block.astype(jnp.float32).reshape(BATCH_SIZE, 6, MODEL_DIM), (2, 1, 1))
    emb_rows = jnp.tile(t_embed.astype(jnp.float32), (2, 1))
    layer_ws = (mod_table, w_qkv, w_proj, w_cq, w_ckv, w_cproj, w_fc1, w_fc2)

    def per_row(row_in):
        hidden_row, caption_row, len_row, t_mods, emb_row = row_in
        key_mask = jnp.arange(TEXT_LEN) < len_row

        def layer_step(residual, layer_w):
            return block_row(residual, caption_row, key_mask, t_mods, layer_w), None

        residual, scan_out = lax.scan(layer_step, hidden_row.astype(jnp.float32), layer_ws)
        shift_scale = final_table.astype(jnp.float32) + emb_row[None, :]
        final_in = (layer_norm(residual) * (1.0 + shift_scale[1]) + shift_scale[0]).astype(jnp.bfloat16)
        out_tok = jnp.dot(final_in, w_out, preferred_element_type=jnp.float32) + b_out.astype(jnp.float32)
        grid_side = LATENT_SIDE // 2
        patches = out_tok.reshape(grid_side, grid_side, 2, 2, 8)[:, :, :, :, :4]
        return patches.transpose(0, 2, 1, 3, 4).reshape(LATENT_SIDE, LATENT_SIDE, 4)

    eps_rows = lax.map(per_row, (hidden, caption, cap_len, t_rows, emb_rows))
    eps_cond = eps_rows[:BATCH_SIZE]
    eps_uncond = eps_rows[BATCH_SIZE:]
    guided = eps_uncond + GUIDANCE * (eps_cond - eps_uncond)
    abar_t = alpha_bar[:, 0][:, None, None, None]
    abar_prev = alpha_bar[:, 1][:, None, None, None]
    x_zero = (x_t - jnp.sqrt(1.0 - abar_t) * guided) / jnp.sqrt(abar_t)
    return jnp.sqrt(abar_prev) * x_zero + jnp.sqrt(1.0 - abar_prev) * guided
```

```python
import functools

import jax
import jax.numpy as jnp
from jax import lax
from jax.experimental import pallas as pl
from jax.experimental.pallas import tpu as pltpu
from jax.sharding import PartitionSpec as P


GUIDANCE = 4.5
LN_EPS = 1e-6
HEAD_DIM = 72
VMEM_LIMIT = 62 * 1024 * 1024
LOG2E = 1.4426950408889634
UNITS = 8
NT = (((1,), (1,)), ((), ()))
TN = (((0,), (0,)), ((), ()))


def layer_norm(values):
    mean_val = jnp.mean(values, axis=-1, keepdims=True)
    centered = values - mean_val
    variance = jnp.mean(centered * centered, axis=-1, keepdims=True)
    return centered * lax.rsqrt(variance + LN_EPS)


def dot32(lhs, rhs, dims):
    return lax.dot_general(lhs, rhs, dims, preferred_element_type=jnp.float32)


def unit_copy(unit_refs, scratch, sems, index, offset, rows):
    array, lead = unit_refs[index]
    src = array.at[lead, pl.ds(offset, rows)] if lead is not None else array.at[pl.ds(offset, rows)]
    return pltpu.make_async_copy(src, scratch.at[pl.ds(index * rows, rows)], sems.at[index])


def unit_list(own, partner, rest):
    return [(own, 0), (own, 1), (partner, 0), (partner, 1)] + [(ref, None) for ref in rest]


def start_units(unit_refs, scratch, sems, offset, rows):
    for index in range(UNITS):
        unit_copy(unit_refs, scratch, sems, index, offset, rows).start()


def wait_units(unit_refs, scratch, sems, offset, rows, first=0, last=UNITS):
    for index in range(first, last):
        unit_copy(unit_refs, scratch, sems, index, offset, rows).wait()


def call(kernel, grid, in_specs, out_specs, out_shape, scratch, flops, nbytes):
    return pl.pallas_call(
        kernel, grid=grid, in_specs=in_specs, out_specs=out_specs, out_shape=out_shape, scratch_shapes=scratch,
        compiler_params=pltpu.CompilerParams(dimension_semantics=('arbitrary',), vmem_limit_bytes=VMEM_LIMIT),
        cost_estimate=pl.CostEstimate(flops=int(flops), bytes_accessed=int(nbytes), transcendentals=0))


ANY = pl.BlockSpec(memory_space=pl.ANY)


def whole(shape):
    return pl.BlockSpec(shape, lambda *_: (0,) * len(shape))


def qkv_kernel(x_ref, mod_ref, own, partner, y, x, ys, xs, out_ref, a_buf, w_buf, sems):
    units = unit_list(own, partner, [y, x, ys, xs])
    rows = own.shape[1]
    step = pl.program_id(0)

    @pl.when(step == 0)
    def _():
        start_units(units, w_buf, sems, 0, rows)

        @pl.loop(0, x_ref.shape[0] // 128)
        def _(chunk):
            sl = pl.ds(pl.multiple_of(chunk * 128, 128), 128)
            vals = layer_norm(x_ref[sl, :].astype(jnp.float32))
            a_buf[sl, :] = (vals * (1.0 + mod_ref[1:2, :]) + mod_ref[0:1, :]).astype(jnp.bfloat16)

    for index in range(UNITS):
        @pl.when(step == index)
        def _():
            unit_copy(units, w_buf, sems, index, 0, rows).wait()
    res = dot32(w_buf[pl.ds(pl.multiple_of(step * rows, 16), rows), :], a_buf[...], NT)
    for j in range(rows // HEAD_DIM):
        out_ref[j] = res[j * HEAD_DIM:(j + 1) * HEAD_DIM].astype(jnp.bfloat16)


def qkv_call(x, mod, units):
    tokens, dim = x.shape
    rows = units[0].shape[1]
    per = rows // HEAD_DIM
    return call(
        qkv_kernel, (UNITS,), [whole((tokens, dim)), whole(mod.shape)] + [ANY] * 6,
        pl.BlockSpec((per, HEAD_DIM, tokens), lambda i: (i, 0, 0)),
        jax.ShapeDtypeStruct((UNITS * per, HEAD_DIM, tokens), jnp.bfloat16),
        [pltpu.VMEM((tokens, dim), jnp.bfloat16), pltpu.VMEM((UNITS * rows, dim), jnp.bfloat16), pltpu.SemaphoreType.DMA((UNITS,))],
        2 * tokens * dim * rows * UNITS, 4 * tokens * dim + 4 * rows * UNITS * dim)(x, mod, *units)


def softmax_out(scores, v_t, scale):
    top = jnp.max(scores, axis=0, keepdims=True)
    prob = jnp.exp2((scores - top) * scale)
    total = jnp.sum(prob, axis=0, keepdims=True)
    return dot32(v_t, prob.astype(jnp.bfloat16), (((1,), (0,)), ((), ()))) * (1.0 / total)


def self_attn_kernel(qkv_ref, out_ref, *, chunk):
    scale = HEAD_DIM ** -0.5 * LOG2E
    tokens = qkv_ref.shape[2]
    keys = [qkv_ref[3 * h + 1].astype(jnp.float32).T.astype(jnp.bfloat16) for h in range(2)]
    vals = [qkv_ref[3 * h + 2] for h in range(2)]
    for start in range(0, tokens, chunk):
        sl = slice(start, start + chunk)
        scores = [dot32(keys[h], qkv_ref[3 * h, :, sl], (((1,), (0,)), ((), ()))) for h in range(2)]
        outs = [softmax_out(scores[h], vals[h], scale) for h in range(2)]
        out_ref[:, sl] = jnp.concatenate(outs, axis=0).astype(jnp.bfloat16)


def self_attn_call(qkv):
    n_vecs, _, tokens = qkv.shape
    heads = n_vecs // 3
    return call(
        functools.partial(self_attn_kernel, chunk=256), (heads // 2,),
        [pl.BlockSpec((6, HEAD_DIM, tokens), lambda i: (i, 0, 0))],
        pl.BlockSpec((2 * HEAD_DIM, tokens), lambda i: (i, 0)),
        jax.ShapeDtypeStruct((heads * HEAD_DIM, tokens), jnp.bfloat16), [],
        heads * 4 * tokens * tokens * 256, n_vecs * HEAD_DIM * tokens * 4)(qkv)


def proj_kernel(o_ref, x_ref, mod_ref, own, partner, y, x, ys, xs, x_out, q_out, p_buf, q_buf, p_sems, q_sems):
    units = unit_list(own, partner, [y, x, ys, xs])
    rows = 2 * HEAD_DIM

    @pl.when(pl.program_id(0) == 0)
    def _():
        start_units(units, p_buf, p_sems, 0, rows)
        start_units(units, q_buf, q_sems, rows, rows)
        wait_units(units, p_buf, p_sems, 0, rows)

    part = dot32(o_ref[...], p_buf[...], TN).astype(jnp.bfloat16).astype(jnp.float32)
    resid = x_ref[...].astype(jnp.float32) + mod_ref[2:3, :] * part
    x_out[...] = resid

    @pl.when(pl.program_id(0) == 0)
    def _():
        wait_units(units, q_buf, q_sems, rows, rows)

    q_t = dot32(q_buf[...], resid.astype(jnp.bfloat16), NT)
    for h in range(q_out.shape[0]):
        q_out[h] = q_t[h * HEAD_DIM:(h + 1) * HEAD_DIM].astype(jnp.bfloat16)


def proj_call(o_t, x, mod, units, chunk=512):
    tokens, dim = x.shape
    heads = UNITS * 2
    return call(
        proj_kernel, (tokens // chunk,),
        [pl.BlockSpec((dim, chunk), lambda i: (0, i)), pl.BlockSpec((chunk, dim), lambda i: (i, 0)), whole(mod.shape)] + [ANY] * 6,
        [pl.BlockSpec((chunk, dim), lambda i: (i, 0)), pl.BlockSpec((heads, HEAD_DIM, chunk), lambda i: (0, 0, i))],
        [jax.ShapeDtypeStruct((tokens, dim), jnp.float32), jax.ShapeDtypeStruct((heads, HEAD_DIM, tokens), jnp.bfloat16)],
        [pltpu.VMEM((dim, dim), jnp.bfloat16)] * 2 + [pltpu.SemaphoreType.DMA((UNITS,))] * 2,
        4 * tokens * dim * dim, 12 * tokens * dim)(o_t, x, mod, *units)


def ckv_kernel(cap_ref, own, partner, y, x, ys, xs, out_ref, w_buf, sems):
    units = unit_list(own, partner, [y, x, ys, xs])
    rows = 4 * HEAD_DIM
    step = pl.program_id(0)

    @pl.when(step == 0)
    def _():
        start_units(units, w_buf, sems, 6 * HEAD_DIM, rows)

    for index in range(UNITS):
        @pl.when(step == index)
        def _():
            unit_copy(units, w_buf, sems, index, 6 * HEAD_DIM, rows).wait()
    res = dot32(w_buf[pl.ds(pl.multiple_of(step * rows, 16), rows), :], cap_ref[...], NT)
    for j in range(4):
        out_ref[j] = res[j * HEAD_DIM:(j + 1) * HEAD_DIM].astype(jnp.bfloat16)


def ckv_call(cap, units):
    text, dim = cap.shape
    return call(
        ckv_kernel, (UNITS,), [whole((text, dim))] + [ANY] * 6,
        pl.BlockSpec((4, HEAD_DIM, text), lambda i: (i, 0, 0)),
        jax.ShapeDtypeStruct((4 * UNITS, HEAD_DIM, text), jnp.bfloat16),
        [pltpu.VMEM((UNITS * 4 * HEAD_DIM, dim), jnp.bfloat16), pltpu.SemaphoreType.DMA((UNITS,))],
        2 * text * dim * 2 * dim, 4 * dim * dim)(cap, *units)


def cross_attn_kernel(len_ref, q_ref, kv_ref, out_ref, *, chunk, text):
    scale = HEAD_DIM ** -0.5 * LOG2E
    tokens = q_ref.shape[2]
    keys = [kv_ref[2 * h].astype(jnp.float32).T[:text].astype(jnp.bfloat16) for h in range(2)]
    vals = [kv_ref[2 * h + 1][:, :text] for h in range(2)]
    live = lax.broadcasted_iota(jnp.int32, (text, chunk), 0) < len_ref[0]
    for start in range(0, tokens, chunk):
        sl = slice(start, start + chunk)
        scores = [dot32(keys[h], q_ref[h, :, sl], (((1,), (0,)), ((), ()))) for h in range(2)]
        outs = [softmax_out(jnp.where(live, scores[h], -1e30), vals[h], scale) for h in range(2)]
        out_ref[:, sl] = jnp.concatenate(outs, axis=0).astype(jnp.bfloat16)


def cross_attn_call(cap_len, q_t, kv_t, text):
    heads, _, tokens = q_t.shape
    return call(
        functools.partial(cross_attn_kernel, chunk=256, text=text), (heads // 2,),
        [pl.BlockSpec(memory_space=pltpu.SMEM), pl.BlockSpec((2, HEAD_DIM, tokens), lambda i: (i, 0, 0)),
         pl.BlockSpec((4, HEAD_DIM, kv_t.shape[2]), lambda i: (i, 0, 0))],
        pl.BlockSpec((2 * HEAD_DIM, tokens), lambda i: (i, 0)),
        jax.ShapeDtypeStruct((heads * HEAD_DIM, tokens), jnp.bfloat16), [],
        heads * 4 * tokens * text * 256, heads * HEAD_DIM * tokens * 4)(cap_len, q_t, kv_t)


def fc1_kernel(o_ref, x_ref, mod_ref, own, partner, y, x, ys, xs, own1, partner1, y1, x1, ys1, xs1, x_out, u_out, p_buf, w_buf, p_sems, w_sems):
    units = unit_list(own, partner, [y, x, ys, xs])
    fc_units = unit_list(own1, partner1, [y1, x1, ys1, xs1])
    rows = 2 * HEAD_DIM
    fc_rows = own1.shape[1]
    first = pl.program_id(0) == 0

    @pl.when(first)
    def _():
        start_units(units, p_buf, p_sems, 2 * rows, rows)
        start_units(fc_units, w_buf, w_sems, 0, fc_rows)
        wait_units(units, p_buf, p_sems, 2 * rows, rows)

    part = dot32(o_ref[...], p_buf[...], TN).astype(jnp.bfloat16).astype(jnp.float32)
    resid = x_ref[...] + part
    x_out[...] = resid
    mlp_in = (layer_norm(resid) * (1.0 + mod_ref[4:5, :]) + mod_ref[3:4, :]).astype(jnp.bfloat16)
    for pair in range(UNITS // 2):
        @pl.when(first)
        def _():
            wait_units(fc_units, w_buf, w_sems, 0, fc_rows, 2 * pair, 2 * pair + 2)

        cols = slice(2 * pair * fc_rows, 2 * (pair + 1) * fc_rows)
        u_out[:, cols] = jax.nn.gelu(dot32(mlp_in, w_buf[cols, :], NT), approximate=True).astype(jnp.bfloat16)


def fc1_call(o_t, x, mod, units, fc_units, chunk=512):
    tokens, dim = x.shape
    hidden = UNITS * fc_units[0].shape[1]
    return call(
        fc1_kernel, (tokens // chunk,),
        [pl.BlockSpec((dim, chunk), lambda i: (0, i)), pl.BlockSpec((chunk, dim), lambda i: (i, 0)), whole(mod.shape)] + [ANY] * 12,
        [pl.BlockSpec((chunk, dim), lambda i: (i, 0)), pl.BlockSpec((chunk, hidden), lambda i: (i, 0))],
        [jax.ShapeDtypeStruct((tokens, dim), jnp.float32), jax.ShapeDtypeStruct((tokens, hidden), jnp.bfloat16)],
        [pltpu.VMEM((dim, dim), jnp.bfloat16), pltpu.VMEM((hidden, dim), jnp.bfloat16)] + [pltpu.SemaphoreType.DMA((UNITS,))] * 2,
        2 * tokens * dim * (dim + hidden), 2 * tokens * hidden + 8 * tokens * dim)(o_t, x, mod, *units, *fc_units)


def fc2_kernel(u_ref, x_ref, mod_ref, own, partner, y, x, ys, xs, *rest):
    units = unit_list(own, partner, [y, x, ys, xs])
    *head, out_ref, w_buf, sems = rest
    rows = own.shape[1]
    half = UNITS // 2 * rows
    first = pl.program_id(0) == 0

    @pl.when(first)
    def _():
        start_units(units, w_buf, sems, 0, rows)
        wait_units(units, w_buf, sems, 0, rows, 0, UNITS // 2)

    total = dot32(u_ref[:, :half], w_buf[:half, :], (((1,), (0,)), ((), ())))

    @pl.when(first)
    def _():
        wait_units(units, w_buf, sems, 0, rows, UNITS // 2, UNITS)

    total = total + dot32(u_ref[:, half:], w_buf[half:, :], (((1,), (0,)), ((), ())))
    resid = x_ref[...] + mod_ref[5:6, :] * total.astype(jnp.bfloat16).astype(jnp.float32)
    if head:
        shift_scale, w_eps, b_eps = head
        final_in = (layer_norm(resid) * (1.0 + shift_scale[1:2, :]) + shift_scale[0:1, :]).astype(jnp.bfloat16)
        out_ref[...] = dot32(w_eps[...], final_in, NT) + b_eps[:, 0:1]
    else:
        out_ref[...] = resid


def fc2_call(u, x, mod, units, head=(), chunk=512):
    tokens, dim = x.shape
    hidden = u.shape[1]
    out_spec = pl.BlockSpec((16, chunk), lambda i: (0, i)) if head else pl.BlockSpec((chunk, dim), lambda i: (i, 0))
    return call(
        fc2_kernel, (tokens // chunk,),
        [pl.BlockSpec((chunk, hidden), lambda i: (i, 0)), pl.BlockSpec((chunk, dim), lambda i: (i, 0)), whole(mod.shape)] + [ANY] * 6 + [whole(h.shape) for h in head],
        out_spec, jax.ShapeDtypeStruct((16, tokens) if head else (tokens, dim), jnp.float32),
        [pltpu.VMEM((hidden, dim), jnp.bfloat16), pltpu.SemaphoreType.DMA((UNITS,))],
        2 * tokens * dim * hidden, 2 * tokens * hidden + 8 * tokens * dim)(u, x, mod, *units, *head)


def local_units(w_qkv, w_proj, w_cq, w_ckv, w_cproj, w_fc1, w_fc2):
    dim = w_qkv.shape[0]

    def halves(weight):
        return weight.reshape(2, -1, dim)

    qkv = halves(w_qkv.transpose(2, 1, 3, 0))
    misc = jnp.concatenate([halves(w_proj), halves(w_cq.transpose(1, 2, 0)), halves(w_cproj), halves(w_ckv.transpose(2, 1, 3, 0))], axis=1)
    return [qkv, misc, halves(w_fc1.T), halves(w_fc2)]


SWAP = [(i, i ^ 1) for i in range(4)]


class Group:
    def __init__(self, own):
        self.own = own
        half = lax.dynamic_index_in_dim(own, lax.axis_index('dp'), 0, keepdims=False)
        self.over_y = lax.ppermute(half, 'tp', [(i, i ^ 2) for i in range(4)])
        self.partner = lax.ppermute(own, 'tp', SWAP)

    def relay(self, tok):
        self.over_y, tok = lax.optimization_barrier((self.over_y, tok))
        self.over_x = lax.ppermute(self.over_y, 'dp', [(0, 1), (1, 0)])
        self.y_swap = lax.ppermute(self.over_y, 'tp', SWAP)
        return tok

    def finish(self, tok):
        self.over_x, tok = lax.optimization_barrier((self.over_x, tok))
        self.x_swap = lax.ppermute(self.over_x, 'tp', SWAP)
        return tok

    def units(self):
        return [self.own, self.partner, self.over_y, self.over_x, self.y_swap, self.x_swap]


def transformer(x, cap, cap_len, mods, groups, head, text):
    n_layers = len(groups)
    x = groups[0][0].relay(x)
    x = groups[0][0].finish(x)
    for layer in range(n_layers):
        qkv_g, misc_g, fc1_g, fc2_g = groups[layer]
        mod = mods[layer]
        following = groups[layer + 1][0] if layer + 1 < n_layers else None
        qkv = qkv_call(x, mod, qkv_g.units())
        qkv = misc_g.relay(qkv)
        o_t = self_attn_call(qkv)
        o_t = misc_g.finish(fc1_g.relay(o_t))
        kv_t = ckv_call(cap, misc_g.units())
        x1, q_t = proj_call(o_t, x, mod, misc_g.units())
        q_t = fc2_g.relay(q_t) if layer else q_t
        oc_t = cross_attn_call(cap_len, q_t, kv_t, text)
        oc_t = fc1_g.finish(oc_t)
        oc_t = oc_t if layer else fc2_g.relay(oc_t)
        x2, hid = fc1_call(oc_t, x1, mod, misc_g.units(), fc1_g.units())
        hid = fc2_g.finish(following.relay(hid) if following else hid)
        if following:
            x = fc2_call(hid, x2, mod, fc2_g.units())
            x = following.finish(x)
    return fc2_call(hid, x2, mod, fc2_g.units(), head)


def ddim_update(guided, x_t, alpha_bar):
    abar_t = alpha_bar[:, 0][:, None, None, None]
    abar_prev = alpha_bar[:, 1][:, None, None, None]
    x_zero = (x_t - jnp.sqrt(1.0 - abar_t) * guided) / jnp.sqrt(abar_t)
    return jnp.sqrt(abar_prev) * x_zero + jnp.sqrt(1.0 - abar_prev) * guided


def solution(mesh):
    row_spec = P(('dp', 'cfg'))
    part_spec = P('dp')
    in_specs = (row_spec, row_spec, row_spec, part_spec, part_spec, part_spec, part_spec, P(),
                P(None, None, None, 'tp'), P(None, 'tp'), P(None, None, 'tp'), P(None, None, None, 'tp'),
                P(None, 'tp'), P(None, None, 'tp'), P(None, 'tp'), P(), P(), P())

    def local_step(hidden, caption, cap_len, t_block, t_embed, x_t, alpha_bar, mod_table, w_qkv, w_proj, w_cq, w_ckv, w_cproj, w_fc1, w_fc2, final_table, w_out, b_out):
        dim = hidden.shape[2]
        n_images = t_block.shape[0]
        tp, cfg = lax.axis_index('tp'), lax.axis_index('cfg')
        image = (cfg * hidden.shape[0] + tp) % n_images
        layers = []
        for layer in range(mod_table.shape[0]):
            own = local_units(w_qkv[layer], w_proj[layer], w_cq[layer], w_ckv[layer], w_cproj[layer], w_fc1[layer], w_fc2[layer])
            layers.append([Group(group) for group in own])
        x = lax.dynamic_index_in_dim(hidden, tp, 0, keepdims=False)
        n_text = caption.shape[1]
        text = -(-n_text // 16) * 16
        cap = jnp.pad(lax.dynamic_index_in_dim(caption, tp, 0, keepdims=False), ((0, -(-n_text // 128) * 128 - n_text), (0, 0)))
        row_len = lax.dynamic_slice_in_dim(cap_len, tp, 1, 0)
        t_mods = lax.dynamic_index_in_dim(t_block, image, 0, keepdims=False).astype(jnp.float32).reshape(6, dim)
        emb = lax.dynamic_index_in_dim(t_embed, image, 0, keepdims=False).astype(jnp.float32)
        mods = [mod_table[layer].astype(jnp.float32) + t_mods for layer in range(mod_table.shape[0])]
        w_eps = w_out.reshape(dim, 4, 8)[:, :, :4].reshape(dim, 16).T
        b_eps = jnp.broadcast_to(b_out.astype(jnp.float32).reshape(4, 8)[:, :4].reshape(16, 1), (16, 128))
        head = (final_table.astype(jnp.float32) + emb[None, :], w_eps, b_eps)
        eps = transformer(x, cap, row_len, mods, layers, head, text)
        other = lax.ppermute(eps, 'cfg', [(i, (i + 2) % 4) for i in range(4)])
        is_cond = cfg < 2
        eps_cond = jnp.where(is_cond, eps, other)
        eps_uncond = jnp.where(is_cond, other, eps)
        guided = eps_uncond + GUIDANCE * (eps_cond - eps_uncond)
        mine = lax.all_gather(guided, 'tp', axis=0)
        theirs = lax.ppermute(mine, 'cfg', [(i, i ^ 1) for i in range(4)])
        even = cfg % 2 == 0
        guided = jnp.concatenate([jnp.where(even, mine, theirs), jnp.where(even, theirs, mine)], axis=0)
        side = x_t.shape[1] // 2
        guided = guided.reshape(n_images, 2, 2, 4, side, side).transpose(0, 4, 1, 5, 2, 3).reshape(x_t.shape)
        return ddim_update(guided, x_t, alpha_bar)

    return jax.shard_map(local_step, mesh=mesh, in_specs=in_specs, out_specs=part_spec, check_vma=False)
```

```python
import functools

import jax
import jax.numpy as jnp
from jax import lax
from jax.experimental import pallas as pl
from jax.experimental.pallas import tpu as pltpu
from jax.sharding import PartitionSpec as P


GUIDANCE = 4.5
LN_EPS = 1e-6
HEAD_DIM = 72
VMEM_LIMIT = 62 * 1024 * 1024
LOG2E = 1.4426950408889634
UNITS = 8
NT = (((1,), (1,)), ((), ()))
NN = (((1,), (0,)), ((), ()))
TN = (((0,), (0,)), ((), ()))


def layer_norm(values):
    mean_val = jnp.mean(values, axis=-1, keepdims=True)
    centered = values - mean_val
    variance = jnp.mean(centered * centered, axis=-1, keepdims=True)
    return centered * lax.rsqrt(variance + LN_EPS)


def dot32(lhs, rhs, dims):
    return lax.dot_general(lhs, rhs, dims, preferred_element_type=jnp.float32)


def unit_copies(group, scratch, sems, parts, base=0):
    layer, own, partner, hops = group
    rows = 2 * HEAD_DIM
    copies = []
    for unit in range(UNITS):
        for index, part in enumerate(parts):
            if unit < 4:
                ref, lead = (own, partner)[unit // 2][part]
                src = ref.at[(layer,) + lead + (pl.ds(unit % 2 * rows, rows),)]
            else:
                src = hops[unit - 4].at[base + index]
            dst = scratch.at[pl.ds((unit * len(parts) + index) * rows, rows)]
            copies.append((unit, pltpu.make_async_copy(src, dst, sems.at[unit])))
    return copies


def shard_copies(layer, own, partner, hops, x_index, scratch, sems):
    dim = own.shape[1]
    half = dim // 2
    copies = []
    for unit in range(UNITS):
        shard = unit // 2
        if unit < 4:
            src, side = (own, partner)[shard].at[layer, pl.ds(unit % 2 * half, half)], unit % 2
        else:
            src, side = hops[unit - 4], (x_index if unit % 2 == 0 else 1 - x_index)
        dst = scratch.at[pl.ds(pl.multiple_of(shard * dim + side * half, 16), half)]
        copies.append(pltpu.make_async_copy(src, dst, sems.at[unit]))
    return copies


def wait_shards(own, scratch, sems, first, count):
    half = own.shape[1] // 2
    for unit in range(count):
        pltpu.make_async_copy(own.at[0, pl.ds(0, half)], scratch.at[pl.ds(0, half)], sems.at[first + unit]).wait()


def call(kernel, grid, in_specs, out_specs, out_shape, scratch, flops, nbytes):
    return pl.pallas_call(
        kernel, out_shape=out_shape,
        grid_spec=pltpu.PrefetchScalarGridSpec(num_scalar_prefetch=1, grid=grid, in_specs=in_specs, out_specs=out_specs, scratch_shapes=scratch),
        compiler_params=pltpu.CompilerParams(dimension_semantics=('arbitrary',), vmem_limit_bytes=VMEM_LIMIT),
        cost_estimate=pl.CostEstimate(flops=int(flops), bytes_accessed=int(nbytes), transcendentals=0))


ANY = pl.BlockSpec(memory_space=pl.ANY)


def whole(shape):
    return pl.BlockSpec(shape, lambda *_: (0,) * len(shape))


def row_spec(x, chunk):
    if x.shape[0] == 1:
        return pl.BlockSpec((None, chunk, x.shape[2]), lambda i, sel: (0, i, 0))
    return pl.BlockSpec((None, chunk, x.shape[2]), lambda i, sel: (sel[0], i, 0))


def whole_row_spec(x):
    if x.shape[0] == 1:
        return pl.BlockSpec((None,) + x.shape[1:], lambda i, sel: (0, 0, 0))
    return pl.BlockSpec((None,) + x.shape[1:], lambda i, sel: (sel[0], 0, 0))


def qkv_kernel(sel_ref, x_ref, mod_ref, own, partner, h0, h1, h2, h3, out_ref, a_buf, w_buf, sems, *, layer):
    step = pl.program_id(0)
    parts = range(3)
    group = (layer, [(own, (p,)) for p in parts], [(partner, (p,)) for p in parts], [h0, h1, h2, h3])
    copies = unit_copies(group, w_buf, sems, parts)
    rows = 6 * HEAD_DIM

    @pl.when(step == 0)
    def _():
        for _, copy in copies:
            copy.start()

        @pl.loop(0, x_ref.shape[0] // 128)
        def _(chunk):
            sl = pl.ds(pl.multiple_of(chunk * 128, 128), 128)
            vals = layer_norm(x_ref[sl, :].astype(jnp.float32))
            a_buf[sl, :] = (vals * (1.0 + mod_ref[1:2, :]) + mod_ref[0:1, :]).astype(jnp.bfloat16)

    for _ in parts:
        pltpu.make_async_copy(own.at[0, 0, pl.ds(0, 2 * HEAD_DIM)], w_buf.at[pl.ds(0, 2 * HEAD_DIM)], sems.at[step]).wait()
    res = dot32(w_buf[pl.ds(pl.multiple_of(step * rows, 16), rows), :], a_buf[...], NT)
    for j in range(6):
        out_ref[j] = res[j * HEAD_DIM:(j + 1) * HEAD_DIM].astype(jnp.bfloat16)


def qkv_call(sel, x, mod, group):
    tokens, dim = x.shape[1:]
    rows = 6 * HEAD_DIM
    return call(
        functools.partial(qkv_kernel, layer=group.layer), (UNITS,),
        [whole_row_spec(x), whole(mod.shape)] + [ANY] * 6,
        pl.BlockSpec((6, HEAD_DIM, tokens), lambda i, sel: (i, 0, 0)),
        jax.ShapeDtypeStruct((UNITS * 6, HEAD_DIM, tokens), jnp.bfloat16),
        [pltpu.VMEM((tokens, dim), jnp.bfloat16), pltpu.VMEM((UNITS * rows, dim), jnp.bfloat16), pltpu.SemaphoreType.DMA((UNITS,))],
        2 * tokens * dim * rows * UNITS, 4 * tokens * dim + 4 * rows * UNITS * dim)(sel, x, mod, *group.own, *group.partner, *group.hops())


def softmax_out(scores, v_t, scale):
    top = jnp.max(scores, axis=0, keepdims=True)
    prob = jnp.exp2((scores - top) * scale)
    total = jnp.sum(prob, axis=0, keepdims=True)
    return dot32(v_t, prob.astype(jnp.bfloat16), NN) * (1.0 / total)


def self_attn_kernel(sel_ref, qkv_ref, out_ref, *, chunk):
    scale = HEAD_DIM ** -0.5 * LOG2E
    tokens = qkv_ref.shape[2]
    keys = [qkv_ref[2 + h].astype(jnp.float32).T.astype(jnp.bfloat16) for h in range(2)]
    vals = [qkv_ref[4 + h] for h in range(2)]
    for start in range(0, tokens, chunk):
        sl = slice(start, start + chunk)
        scores = [dot32(keys[h], qkv_ref[h, :, sl], NN) for h in range(2)]
        outs = [softmax_out(scores[h], vals[h], scale) for h in range(2)]
        out_ref[:, sl] = jnp.concatenate(outs, axis=0).astype(jnp.bfloat16)


def self_attn_call(sel, qkv):
    n_vecs, _, tokens = qkv.shape
    heads = n_vecs // 3
    return call(
        functools.partial(self_attn_kernel, chunk=256), (heads // 2,),
        [pl.BlockSpec((6, HEAD_DIM, tokens), lambda i, sel: (i, 0, 0))],
        pl.BlockSpec((2 * HEAD_DIM, tokens), lambda i, sel: (i, 0)),
        jax.ShapeDtypeStruct((heads * HEAD_DIM, tokens), jnp.bfloat16), [],
        heads * 4 * tokens * tokens * 256, n_vecs * HEAD_DIM * tokens * 4)(sel, qkv)


def misc_group(layer, proj, cq, cproj, ckv, proj_p, cq_p, cproj_p, ckv_p, hops):
    own = [(proj, ()), (cq, ()), (cproj, ()), (ckv, (0,)), (ckv, (1,))]
    partner = [(proj_p, ()), (cq_p, ()), (cproj_p, ()), (ckv_p, (0,)), (ckv_p, (1,))]
    return layer, own, partner, hops


def start_all(copies):
    for _, copy in copies:
        copy.start()


def wait_all(copies):
    for _, copy in copies:
        copy.wait()


def proj_kernel(sel_ref, o_ref, x_ref, mod_ref, proj, cq, cproj, ckv, proj_p, cq_p, cproj_p, ckv_p, h0, h1, h2, h3, x_out, q_out, p_buf, q_buf, p_sems, q_sems, *, layer):
    group = misc_group(layer, proj, cq, cproj, ckv, proj_p, cq_p, cproj_p, ckv_p, [h0, h1, h2, h3])
    p_copies = unit_copies(group, p_buf, p_sems, [0], 0)
    q_copies = unit_copies(group, q_buf, q_sems, [1], 1)

    @pl.when(pl.program_id(0) == 0)
    def _():
        start_all(p_copies)
        start_all(q_copies)
        wait_all(p_copies)

    part = dot32(o_ref[...], p_buf[...], TN).astype(jnp.bfloat16).astype(jnp.float32)
    resid = x_ref[...].astype(jnp.float32) + mod_ref[2:3, :] * part
    x_out[...] = resid

    @pl.when(pl.program_id(0) == 0)
    def _():
        wait_all(q_copies)

    q_t = dot32(q_buf[...], resid.astype(jnp.bfloat16), NT)
    for h in range(q_out.shape[0]):
        q_out[h] = q_t[h * HEAD_DIM:(h + 1) * HEAD_DIM].astype(jnp.bfloat16)


def proj_call(sel, o_t, x, mod, group, chunk=512):
    tokens, dim = x.shape[1:]
    heads = UNITS * 2
    return call(
        functools.partial(proj_kernel, layer=group.layer), (tokens // chunk,),
        [pl.BlockSpec((dim, chunk), lambda i, sel: (0, i)), row_spec(x, chunk), whole(mod.shape)] + [ANY] * 12,
        [pl.BlockSpec((None, chunk, dim), lambda i, sel: (0, i, 0)), pl.BlockSpec((heads, HEAD_DIM, chunk), lambda i, sel: (0, 0, i))],
        [jax.ShapeDtypeStruct((1, tokens, dim), jnp.float32), jax.ShapeDtypeStruct((heads, HEAD_DIM, tokens), jnp.bfloat16)],
        [pltpu.VMEM((dim, dim), jnp.bfloat16)] * 2 + [pltpu.SemaphoreType.DMA((UNITS,))] * 2,
        4 * tokens * dim * dim, 12 * tokens * dim)(sel, o_t, x, mod, *group.own, *group.partner, *group.hops())


def ckv_kernel(sel_ref, cap_ref, proj, cq, cproj, ckv, proj_p, cq_p, cproj_p, ckv_p, h0, h1, h2, h3, out_ref, w_buf, sems, *, layer):
    group = misc_group(layer, proj, cq, cproj, ckv, proj_p, cq_p, cproj_p, ckv_p, [h0, h1, h2, h3])
    copies = unit_copies(group, w_buf, sems, [3, 4], 3)
    rows = 4 * HEAD_DIM
    step = pl.program_id(0)

    @pl.when(step == 0)
    def _():
        start_all(copies)

    for _ in range(2):
        pltpu.make_async_copy(proj.at[0, pl.ds(0, 2 * HEAD_DIM)], w_buf.at[pl.ds(0, 2 * HEAD_DIM)], sems.at[step]).wait()
    res = dot32(w_buf[pl.ds(pl.multiple_of(step * rows, 16), rows), :], cap_ref[...], NT)
    for j in range(4):
        out_ref[j] = res[j * HEAD_DIM:(j + 1) * HEAD_DIM].astype(jnp.bfloat16)


def ckv_call(sel, cap, group):
    text, dim = cap.shape
    return call(
        functools.partial(ckv_kernel, layer=group.layer), (UNITS,), [whole((text, dim))] + [ANY] * 12,
        pl.BlockSpec((4, HEAD_DIM, text), lambda i, sel: (i, 0, 0)),
        jax.ShapeDtypeStruct((4 * UNITS, HEAD_DIM, text), jnp.bfloat16),
        [pltpu.VMEM((UNITS * 4 * HEAD_DIM, dim), jnp.bfloat16), pltpu.SemaphoreType.DMA((UNITS,))],
        4 * text * dim * dim, 4 * dim * dim)(sel, cap, *group.own, *group.partner, *group.hops())


def cross_attn_kernel(sel_ref, q_ref, kv_ref, out_ref, *, chunk, text):
    scale = HEAD_DIM ** -0.5 * LOG2E
    tokens = q_ref.shape[2]
    keys = [kv_ref[h].astype(jnp.float32).T[:text].astype(jnp.bfloat16) for h in range(2)]
    vals = [kv_ref[2 + h][:, :text] for h in range(2)]
    live = lax.broadcasted_iota(jnp.int32, (text, chunk), 0) < sel_ref[2]
    for start in range(0, tokens, chunk):
        sl = slice(start, start + chunk)
        scores = [dot32(keys[h], q_ref[h, :, sl], NN) for h in range(2)]
        outs = [softmax_out(jnp.where(live, scores[h], -1e30), vals[h], scale) for h in range(2)]
        out_ref[:, sl] = jnp.concatenate(outs, axis=0).astype(jnp.bfloat16)


def cross_attn_call(sel, q_t, kv_t, text):
    heads, _, tokens = q_t.shape
    return call(
        functools.partial(cross_attn_kernel, chunk=256, text=text), (heads // 2,),
        [pl.BlockSpec((2, HEAD_DIM, tokens), lambda i, sel: (i, 0, 0)), pl.BlockSpec((4, HEAD_DIM, kv_t.shape[2]), lambda i, sel: (i, 0, 0))],
        pl.BlockSpec((2 * HEAD_DIM, tokens), lambda i, sel: (i, 0)),
        jax.ShapeDtypeStruct((heads * HEAD_DIM, tokens), jnp.bfloat16), [],
        heads * 4 * tokens * text * 256, heads * HEAD_DIM * tokens * 4)(sel, q_t, kv_t)


def fc1_kernel(sel_ref, o_ref, x_ref, mod_ref, proj, cq, cproj, ckv, proj_p, cq_p, cproj_p, ckv_p, h0, h1, h2, h3,
               own, partner, g0, g1, g2, g3, x_out, u_out, p_buf, w_buf, p_sems, w_sems, *, layer):
    group = misc_group(layer, proj, cq, cproj, ckv, proj_p, cq_p, cproj_p, ckv_p, [h0, h1, h2, h3])
    p_copies = unit_copies(group, p_buf, p_sems, [2], 2)
    w_copies = shard_copies(layer, own, partner, [g0, g1, g2, g3], sel_ref[1], w_buf, w_sems)
    first = pl.program_id(0) == 0
    dim = own.shape[1]

    @pl.when(first)
    def _():
        start_all(p_copies)
        for copy in w_copies:
            copy.start()
        wait_all(p_copies)

    part = dot32(o_ref[...], p_buf[...], TN).astype(jnp.bfloat16).astype(jnp.float32)
    resid = x_ref[...] + part
    x_out[...] = resid
    mlp_in = (layer_norm(resid) * (1.0 + mod_ref[4:5, :]) + mod_ref[3:4, :]).astype(jnp.bfloat16)
    for shard in range(4):
        @pl.when(first)
        def _():
            wait_shards(own, w_buf, w_sems, 2 * shard, 2)

        cols = slice(shard * dim, (shard + 1) * dim)
        u_out[:, cols] = jax.nn.gelu(dot32(mlp_in, w_buf[cols, :], NN), approximate=True).astype(jnp.bfloat16)


def fc1_call(sel, o_t, x, mod, group, fc_group, chunk=512):
    tokens, dim = x.shape[1:]
    hidden = 4 * dim
    return call(
        functools.partial(fc1_kernel, layer=group.layer), (tokens // chunk,),
        [pl.BlockSpec((dim, chunk), lambda i, sel: (0, i)), row_spec(x, chunk), whole(mod.shape)] + [ANY] * 18,
        [pl.BlockSpec((None, chunk, dim), lambda i, sel: (0, i, 0)), pl.BlockSpec((chunk, hidden), lambda i, sel: (i, 0))],
        [jax.ShapeDtypeStruct((1, tokens, dim), jnp.float32), jax.ShapeDtypeStruct((tokens, hidden), jnp.bfloat16)],
        [pltpu.VMEM((dim, dim), jnp.bfloat16), pltpu.VMEM((hidden, dim), jnp.bfloat16)] + [pltpu.SemaphoreType.DMA((UNITS,))] * 2,
        2 * tokens * dim * (dim + hidden), 2 * tokens * hidden + 8 * tokens * dim)(
            sel, o_t, x, mod, *group.own, *group.partner, *group.hops(), *fc_group.own, *fc_group.partner, *fc_group.hops())


def interleave(even, odd):
    lanes = even.shape[1]
    source = lax.broadcasted_iota(jnp.int32, (lanes, 2 * lanes), 0)
    target = lax.broadcasted_iota(jnp.int32, (lanes, 2 * lanes), 1)
    total = None
    for side, values in enumerate((even, odd)):
        place = (target == 2 * source + side).astype(jnp.float32).astype(jnp.bfloat16)
        for _ in range(3):
            piece = values.astype(jnp.bfloat16)
            moved = dot32(piece, place, NN)
            total = moved if total is None else total + moved
            values = values - piece.astype(jnp.float32)
    return total


def fc2_kernel(sel_ref, u_ref, x_ref, mod_ref, own, partner, g0, g1, g2, g3, *rest, layer):
    *head, out_ref, w_buf, sems = rest
    copies = shard_copies(layer, own, partner, [g0, g1, g2, g3], sel_ref[1], w_buf, sems)
    half = 2 * own.shape[1]
    first = pl.program_id(0) == 0

    @pl.when(first)
    def _():
        for copy in copies:
            copy.start()
        wait_shards(own, w_buf, sems, 0, 4)

    total = dot32(u_ref[:, :half], w_buf[:half, :], NN)

    @pl.when(first)
    def _():
        wait_shards(own, w_buf, sems, 4, 4)

    total = total + dot32(u_ref[:, half:], w_buf[half:, :], NN)
    resid = x_ref[...] + mod_ref[5:6, :] * total.astype(jnp.bfloat16).astype(jnp.float32)
    if head:
        shift_scale, w_eps, b_eps = head
        final_in = (layer_norm(resid) * (1.0 + shift_scale[1:2, :]) + shift_scale[0:1, :]).astype(jnp.bfloat16)
        eps = dot32(w_eps[...], final_in, NT) + b_eps[:, 0:1]
        for start in range(0, eps.shape[1], 128):
            out_ref[:, 2 * start:2 * start + 256] = interleave(eps[:8, start:start + 128], eps[8:, start:start + 128])
    else:
        out_ref[...] = resid


def fc2_call(sel, u, x, mod, group, head=(), chunk=512):
    tokens, dim = x.shape[1:]
    hidden = u.shape[1]
    out_spec = pl.BlockSpec((8, 2 * chunk), lambda i, sel: (0, i)) if head else pl.BlockSpec((None, chunk, dim), lambda i, sel: (0, i, 0))
    return call(
        functools.partial(fc2_kernel, layer=group.layer), (tokens // chunk,),
        [pl.BlockSpec((chunk, hidden), lambda i, sel: (i, 0)), row_spec(x, chunk), whole(mod.shape)] + [ANY] * 6 + [whole(h.shape) for h in head],
        out_spec, jax.ShapeDtypeStruct((8, 2 * tokens) if head else (1, tokens, dim), jnp.float32),
        [pltpu.VMEM((hidden, dim), jnp.bfloat16), pltpu.SemaphoreType.DMA((UNITS,))],
        2 * tokens * dim * hidden, 2 * tokens * hidden + 8 * tokens * dim)(sel, u, x, mod, *group.own, *group.partner, *group.hops(), *head)


SWAP = [(i, i ^ 1) for i in range(4)]


class Group:
    def __init__(self, layer, own, partner, half):
        self.layer, self.own, self.partner = layer, own, partner
        self.over_y = lax.ppermute(half, 'tp', [(i, i ^ 2) for i in range(4)])

    def relay(self, tok):
        self.over_y, tok = lax.optimization_barrier((self.over_y, tok))
        self.over_x = lax.ppermute(self.over_y, 'dp', [(0, 1), (1, 0)])
        self.y_swap = lax.ppermute(self.over_y, 'tp', SWAP)
        return tok

    def finish(self, tok):
        self.over_x, tok = lax.optimization_barrier((self.over_x, tok))
        self.x_swap = lax.ppermute(self.over_x, 'tp', SWAP)
        return tok

    def hops(self):
        return [self.over_y, self.over_x, self.y_swap, self.x_swap]


def weight_groups(w_qkv, w_proj, w_cq, w_ckv, w_cproj, w_fc1, w_fc2):
    n_layers, dim = w_qkv.shape[:2]
    side = lax.axis_index('dp')
    qkv = w_qkv.transpose(0, 2, 3, 4, 1).reshape(n_layers, 3, -1, dim)
    misc = [w_proj.reshape(n_layers, -1, dim), w_cq.transpose(0, 2, 3, 1).reshape(n_layers, -1, dim), w_cproj.reshape(n_layers, -1, dim),
            w_ckv.transpose(0, 2, 3, 4, 1).reshape(n_layers, 2, -1, dim)]
    sets = [[qkv], misc, [w_fc1], [w_fc2]]
    partners = []
    for arrays in sets:
        partners.append([])
        for array in arrays:
            partners[-1].append(lax.ppermute(array, 'tp', SWAP))

    def half(array, layer):
        rows = array.shape[-2] // 2
        starts = (layer,) + (0,) * (array.ndim - 3) + (side * rows, 0)
        return lax.dynamic_slice(array, starts, (1,) + array.shape[1:-2] + (rows, dim))[0]

    layers = []
    for layer in range(n_layers):
        halves = [half(qkv, layer), jnp.concatenate([half(array, layer).reshape(-1, 2 * HEAD_DIM, dim) for array in misc]),
                  half(w_fc1, layer), half(w_fc2, layer)]
        layers.append([Group(layer, sets[index], partners[index], halves[index]) for index in range(4)])
    return layers


def transformer(sel, x, cap, mods, groups, head, text):
    n_layers = len(groups)
    x = groups[0][0].relay(x)
    x = groups[0][0].finish(x)
    for layer in range(n_layers):
        qkv_g, misc_g, fc1_g, fc2_g = groups[layer]
        mod = mods[layer]
        following = groups[layer + 1][0] if layer + 1 < n_layers else None
        qkv = qkv_call(sel, x, mod, qkv_g)
        qkv = misc_g.relay(qkv)
        o_t = self_attn_call(sel, qkv)
        o_t = misc_g.finish(fc1_g.relay(o_t))
        kv_t = ckv_call(sel, cap, misc_g)
        x1, q_t = proj_call(sel, o_t, x, mod, misc_g)
        q_t = fc2_g.relay(q_t) if layer else q_t
        oc_t = cross_attn_call(sel, q_t, kv_t, text)
        oc_t = fc1_g.finish(oc_t)
        oc_t = oc_t if layer else fc2_g.relay(oc_t)
        x2, hid = fc1_call(sel, oc_t, x1, mod, misc_g, fc1_g)
        hid = fc2_g.finish(following.relay(hid) if following else hid)
        if following:
            x = fc2_call(sel, hid, x2, mod, fc2_g)
            x = following.finish(x)
    return fc2_call(sel, hid, x2, mod, fc2_g, head)


def ddim_update(guided, x_t, alpha_bar):
    abar_t = alpha_bar[:, 0][:, None, None, None]
    abar_prev = alpha_bar[:, 1][:, None, None, None]
    x_zero = (x_t - jnp.sqrt(1.0 - abar_t) * guided) / jnp.sqrt(abar_t)
    return jnp.sqrt(abar_prev) * x_zero + jnp.sqrt(1.0 - abar_prev) * guided


def solution(mesh):
    row_spec = P(('dp', 'cfg'))
    part_spec = P('dp')
    in_specs = (row_spec, row_spec, row_spec, part_spec, part_spec, part_spec, part_spec, P(),
                P(None, None, None, 'tp'), P(None, 'tp'), P(None, None, 'tp'), P(None, None, None, 'tp'),
                P(None, 'tp'), P(None, None, 'tp'), P(None, 'tp'), P(), P(), P())

    def local_step(hidden, caption, cap_len, t_block, t_embed, x_t, alpha_bar, mod_table, w_qkv, w_proj, w_cq, w_ckv, w_cproj, w_fc1, w_fc2, final_table, w_out, b_out):
        dim = hidden.shape[2]
        n_images = t_block.shape[0]
        tp, cfg = lax.axis_index('tp'), lax.axis_index('cfg')
        image = (cfg * hidden.shape[0] + tp) % n_images
        layers = weight_groups(w_qkv, w_proj, w_cq, w_ckv, w_cproj, w_fc1, w_fc2)
        n_text = caption.shape[1]
        text = -(-n_text // 16) * 16
        cap = jnp.pad(lax.dynamic_index_in_dim(caption, tp, 0, keepdims=False), ((0, -(-n_text // 128) * 128 - n_text), (0, 0)))
        sel = jnp.stack([tp, lax.axis_index('dp'), lax.dynamic_index_in_dim(cap_len, tp, 0, keepdims=False)]).astype(jnp.int32)
        t_mods = lax.dynamic_index_in_dim(t_block, image, 0, keepdims=False).astype(jnp.float32).reshape(6, dim)
        emb = lax.dynamic_index_in_dim(t_embed, image, 0, keepdims=False).astype(jnp.float32)
        mods = [mod_table[layer].astype(jnp.float32) + t_mods for layer in range(mod_table.shape[0])]
        w_eps = w_out.reshape(dim, 2, 2, 8)[..., :4].transpose(2, 1, 3, 0).reshape(16, dim)
        b_eps = jnp.broadcast_to(b_out.astype(jnp.float32).reshape(2, 2, 8)[..., :4].transpose(1, 0, 2).reshape(16, 1), (16, 128))
        head = (final_table.astype(jnp.float32) + emb[None, :], w_eps, b_eps)
        eps = transformer(sel, hidden, cap, mods, layers, head, text)
        other = lax.ppermute(eps, 'cfg', [(i, (i + 2) % 4) for i in range(4)])
        is_cond = cfg < 2
        eps_cond = jnp.where(is_cond, eps, other)
        eps_uncond = jnp.where(is_cond, other, eps)
        guided = eps_uncond + GUIDANCE * (eps_cond - eps_uncond)
        mine = lax.all_gather(guided, 'tp', axis=0)
        theirs = lax.ppermute(mine, 'cfg', [(i, i ^ 1) for i in range(4)])
        even = cfg % 2 == 0
        guided = jnp.concatenate([jnp.where(even, mine, theirs), jnp.where(even, theirs, mine)], axis=0)
        side = x_t.shape[1] // 2
        guided = guided.reshape(n_images, 2, 4, side, 2 * side).transpose(0, 3, 1, 4, 2).reshape(x_t.shape)
        return ddim_update(guided, x_t, alpha_bar)

    return jax.shard_map(local_step, mesh=mesh, in_specs=in_specs, out_specs=part_spec, check_vma=False)
```
